32 devices in a mesh: rows: 8 (over z, y), feat: 4 (over x, core).
Axes of the slice: x: 2, y: 2, z: 4, core: 2. Of those that a mesh axis runs over, the one named last changes fastest.
Arguments:
- features: float32 [100, 8192], P('feat', 'rows'), may hold values from -12 to 12
- tiles: float32 [1024, 128, 128], P('rows'), may hold values from 0 to 1.5
- tile_slot: int32 [1024], P('rows'), may hold values from 0 to 15, as said below
- send_blocks: int32 [8, 8, 1], P('rows'), may hold values from 0 to 7
Outputs:
- ranked: float32 [100, 8192], P('feat', 'rows')
- change: float32 [4], replicated
The draws below stay inside these ranges and needn't reach their ends.
Inputs may be any that keep to these rules, and one draw needn't show every extreme that they name: `tile_slot`: among the tiles of one index of rows, every received slot (8 to 15) is named by at least one tile.
All inputs are finite; a program needn't handle non-finite values.
Results may differ from the reference program's by a relative error of at most 0.0001.
Values sent between devices are 32-bit elements; how exact they have to be, the bound alone decides.
No kernel may reach another device: no remote copies, remote signals or barrier semaphores. Data moves between devices by JAX's collectives and lax.ppermute only.
A program may use at most 128 MiB of HBM per device.

```python
import jax
import jax.numpy as jnp
from jax import lax

F = 100
TILE = 128
NB = 8
TPB = 16
SLOTS = 1
ITERS = 4
PEERS = 8
NBLK = 64
NODES = 8192


own_rate = 6.0


halo_rate = 1.5


def slot_plan(key):
    base_key = jax.random.fold_in(key, 7101)
    rank_key, choose_key, local_key, remote_key = jax.random.split(base_key, 4)
    per_device = NB * TPB
    halo_count = PEERS * SLOTS
    ordered = jnp.tile(jnp.arange(per_device, dtype=jnp.int32)[None, :], (PEERS, 1))
    ranking = jax.random.permutation(rank_key, ordered, axis=1, independent=True)
    chooser = jax.random.randint(choose_key, (PEERS, per_device), 0, 4, dtype=jnp.int32)
    local_pick = jax.random.randint(local_key, (PEERS, per_device), 0, NB, dtype=jnp.int32)
    remote_pick = jax.random.randint(remote_key, (PEERS, per_device), NB, NB + halo_count, dtype=jnp.int32)
    drawn_slot = jnp.where(chooser == 0, remote_pick, local_pick)
    slot_table = jnp.where(ranking < halo_count, NB + ranking, drawn_slot)
    return slot_table.reshape(PEERS * per_device).astype(jnp.int32)


def draw_tile_slot(key, part):
    return slot_plan(key)


def draw_tiles(key, part):
    slot_table = slot_plan(key)
    local_tile = slot_table < NB
    density = jnp.minimum(jnp.where(local_tile, own_rate, halo_rate) / TILE, 0.9)
    mask_key, weight_key = jax.random.split(jax.random.fold_in(key, 7202))
    chance = jax.random.uniform(mask_key, (NBLK * TPB, TILE, TILE), jnp.float32)
    weights = jax.random.uniform(weight_key, (NBLK * TPB, TILE, TILE), jnp.float32, 0.5, 1.5)
    return jnp.where(chance < density[:, None, None], weights, 0.0).astype(jnp.float32)


def draw_features(key, part):
    base_key = jax.random.fold_in(key, 3301)
    noise_key, device_key, block_key, scale_key = jax.random.split(base_key, 4)
    device_part = jnp.repeat(jax.random.normal(device_key, (F, PEERS, 1), jnp.float32), NB, axis=1)
    block_part = jax.random.normal(block_key, (F, NBLK, 1), jnp.float32)
    noise = jax.random.normal(noise_key, (F, NBLK, TILE), jnp.float32)
    values = noise + 1.5 * device_part + 0.7 * block_part
    return jnp.clip(values, -12.0, 12.0).reshape(F, NODES).astype(jnp.float32)


def with_ends(result, key, least, largest):
    dims = result.shape
    spot = [jax.random.randint(jax.random.fold_in(key, axis), (), 0, dims[axis]) for axis in range(len(dims))]
    result = result.at[tuple(spot)].set(least)
    longest = dims.index(max(dims))
    spot[longest] = (spot[longest] + 1) % dims[longest]
    return result.at[tuple(spot)].set(largest)


def setup_inputs(seed: int = 0) -> dict:
    keys = jax.random.split(jax.random.key(seed), 5)
    return {
        "features": draw_features(jax.random.fold_in(keys[4], 71), 0),
        "tiles": draw_tiles(jax.random.fold_in(keys[4], 71), 0),
        "tile_slot": draw_tile_slot(jax.random.fold_in(keys[4], 71), 0),
        "send_blocks": with_ends(jax.random.randint(keys[3], (PEERS, PEERS, SLOTS), 0, NB), jax.random.fold_in(keys[3], 1), 0, NB - 1).astype(jnp.int32),
    }


teleport = 0.15


def reference(features, tiles, tile_slot, send_blocks):
    total_tiles = NBLK * TPB
    owner = jnp.arange(total_tiles, dtype=jnp.int32) // (NB * TPB)
    remote = jnp.maximum(tile_slot - NB, 0).astype(jnp.int32)
    source = remote // SLOTS
    within = remote % SLOTS
    column = jnp.where(tile_slot < NB, owner * NB + tile_slot, source * NB + send_blocks[source, owner, within]).astype(jnp.int32)
    degree = 1.0 + jnp.sum(tiles, axis=2).reshape(NBLK, TPB, TILE).sum(axis=1).reshape(NODES)
    current = features
    changes = []
    for iteration in range(ITERS):
        blocks = current.reshape(F, NBLK, TILE)
        picked = blocks[:, column, :]
        product = jnp.einsum("tij,ftj->fti", tiles, picked, precision=lax.Precision.HIGHEST)
        summed = product.reshape(F, NBLK, TPB, TILE).sum(axis=2).reshape(F, NODES)
        updated = (1.0 - teleport) * (current + summed) / degree[None, :] + teleport * features
        changes.append(jnp.sum((updated - current) ** 2) / (F * NODES))
        current = updated
    return current, jnp.stack(changes)
```

```python
import jax
import jax.numpy as jnp
from jax import lax
from jax.experimental import pallas as pl
from jax.experimental.pallas import tpu as pltpu
from jax.sharding import PartitionSpec as P

ITERS = 4


teleport = 0.15

VMEM, SMEM = pltpu.VMEM, pltpu.SMEM
WHOLE = pl.BlockSpec(memory_space=VMEM)
SCALARS = pl.BlockSpec(memory_space=SMEM)
LIMIT = pltpu.CompilerParams(vmem_limit_bytes=20 * 1024 * 1024)


def framed(block, rows):
    width, tile = block.shape
    row = lax.broadcasted_iota(jnp.int32, (rows - width, tile), 0)
    return jnp.concatenate([block, jnp.where(row == 0, 1.0, 0.0).astype(block.dtype)], axis=0)


def split(v):
    high = v.astype(jnp.bfloat16)
    return high, (v - high.astype(jnp.float32)).astype(jnp.bfloat16)


def begin_kernel(features_ref, ids_ref, start_ref, outgoing_ref):
    blocks, rows, tile = start_ref.shape
    width = features_ref.shape[0]
    for b in range(blocks):
        start_ref[b] = framed(features_ref[:, b * tile:(b + 1) * tile], rows)
    for d in range(outgoing_ref.shape[0]):
        at = pl.multiple_of(ids_ref[d] * tile, tile)
        outgoing_ref[d] = features_ref[:, pl.ds(at, tile)]


def step_kernel(index, refs):
    first, last = index == 0, index == ITERS - 1
    refs = list(refs)
    current_ref, received_ref, start_ref, slot_ref, ids_ref = refs[:5]
    views_ref = refs.pop()
    if first:
        tiles_ref, next_ref, outgoing_ref, sums_ref, scale_ref, weights_ref = refs[5:]
    elif last:
        scale_ref, weights_ref, past_ref, ranked_ref, sums_ref = refs[5:]
    else:
        scale_ref, weights_ref, past_ref, next_ref, outgoing_ref, sums_ref = refs[5:]
    blocks, rows, tile = current_ref.shape
    width = received_ref.shape[1]
    per_block = weights_ref.shape[0] // (blocks * tile)
    for c in range(blocks + received_ref.shape[0]):
        v = current_ref[c] if c < blocks else framed(received_ref[c - blocks], rows)
        views_ref[c, 0:rows], views_ref[c, rows:2 * rows] = split(v)
    square = jnp.zeros((8, tile), jnp.float32)
    for b in range(blocks):
        if first:
            for t in range(b * per_block, (b + 1) * per_block):
                high, low = split(tiles_ref[t].T)
                weights_ref[t * tile:(t + 1) * tile, 0:tile] = high
                weights_ref[t * tile:(t + 1) * tile, tile:2 * tile] = low
        picked = [views_ref[slot_ref[t]] for t in range(b * per_block, (b + 1) * per_block)]
        s = jnp.dot(
            jnp.concatenate(picked, axis=1),
            weights_ref[b * per_block * tile:(b + 1) * per_block * tile, :],
            preferred_element_type=jnp.float32,
        )
        s = s[0:rows] + s[rows:2 * rows]
        s = s[:, 0:tile] + s[:, tile:2 * tile]
        r = slice(b * tile, (b + 1) * tile)
        if first:
            scale = (1.0 - teleport) / (1.0 + s[width:width + 1])
            scale_ref[:, r] = scale
        else:
            scale = scale_ref[:, r]
        old = current_ref[b]
        new = (old + s) * scale + teleport * start_ref[b]
        row = lax.broadcasted_iota(jnp.int32, (rows, tile), 0)
        new = jnp.where(row < width, new, start_ref[b])
        d = new - old
        d = d * d
        for k in range(rows // 8):
            square = square + d[8 * k:8 * k + 8]
        if last:
            ranked_ref[:, r] = new[0:width]
        else:
            next_ref[b] = new
    row = lax.broadcasted_iota(jnp.int32, (8, tile), 0)
    sums = jnp.where(row == index, jnp.sum(square, axis=0, keepdims=True), 0.0 if first else past_ref[...])
    if last:
        lane = lax.broadcasted_iota(jnp.int32, (8, tile), 1)
        sums = jnp.where(row == lane, jnp.sum(sums, axis=1, keepdims=True), 0.0)
        sums_ref[...] = jnp.broadcast_to(jnp.sum(sums, axis=0, keepdims=True), sums_ref.shape)
    else:
        sums_ref[...] = sums
    if not last:
        for d in range(outgoing_ref.shape[0]):
            outgoing_ref[d] = next_ref[ids_ref[d], 0:width]


def shards(features, tiles, tile_slot, send_blocks):
    width, node_count = features.shape
    tile_count, tile, _ = tiles.shape
    blocks = node_count // tile
    peers = lax.axis_size("rows")
    lanes = lax.axis_size("feat")
    halo = peers * send_blocks.shape[2]
    rows = -(-(width + 1) // 8) * 8
    f32 = jnp.float32
    ids = send_blocks.reshape(-1)
    shape = jax.ShapeDtypeStruct

    start, outgoing = pl.pallas_call(
        begin_kernel,
        out_shape=(shape((blocks, rows, tile), f32), shape((halo, width, tile), f32)),
        in_specs=[WHOLE, SCALARS],
        out_specs=(WHOLE, WHOLE),
        compiler_params=LIMIT,
        cost_estimate=pl.CostEstimate(flops=20_000_000_000, bytes_accessed=20_000_000, transcendentals=0),
        name="begin",
    )(features, ids)

    current = start
    everyone = peers * lanes
    for i in range(ITERS):
        first, last = i == 0, i == ITERS - 1
        received = lax.all_to_all(outgoing, "rows", split_axis=0, concat_axis=0, tiled=True)
        if last:
            outs = [shape((width, node_count), f32), shape((everyone, tile), f32)]
        else:
            outs = [shape((blocks, rows, tile), f32), shape((halo, width, tile), f32), shape((8, tile), f32)]
        if first:
            outs += [shape((1, node_count), f32), VMEM((tile_count * tile, 2 * tile), jnp.bfloat16)]
        kept = (tiles,) if first else (scale, weights, sums)
        got = pl.pallas_call(
            lambda *refs, i=i: step_kernel(i, refs),
            out_shape=tuple(outs),
            in_specs=[WHOLE] * 3 + [SCALARS] * 2 + [WHOLE] * len(kept),
            out_specs=(WHOLE,) * len(outs),
            scratch_shapes=[VMEM((blocks + halo, 2 * rows, tile), jnp.bfloat16)],
            compiler_params=LIMIT,
            name=f"step{i}",
        )(current, received, start, tile_slot, ids, *kept)
        if first:
            current, outgoing, sums, scale, weights = got
            weights = pltpu.with_memory_space_constraint(weights, VMEM)
        elif last:
            ranked, sums = got
        else:
            current, outgoing, sums = got
    theirs = lax.all_to_all(sums, ("rows", "feat"), split_axis=0, concat_axis=0, tiled=True)
    change = jnp.sum(theirs, axis=0)[:ITERS] / (width * lanes * node_count * peers)
    return ranked, change


def solution(mesh):
    return jax.shard_map(
        shards,
        mesh=mesh,
        in_specs=(P("feat", "rows"), P("rows", None, None), P("rows"), P("rows", None, None)),
        out_specs=(P("feat", "rows"), P()),
        check_vma=False,
    )
```

```python
import jax
import jax.numpy as jnp
from jax import lax
from jax.experimental import pallas as pl
from jax.experimental.pallas import tpu as pltpu
from jax.sharding import PartitionSpec as P

ITERS = 4


teleport = 0.15

VMEM, SMEM = pltpu.VMEM, pltpu.SMEM
WHOLE = pl.BlockSpec(memory_space=VMEM)
SCALARS = pl.BlockSpec(memory_space=SMEM)
LIMIT = pltpu.CompilerParams(vmem_limit_bytes=20 * 1024 * 1024)


def framed(block, rows):
    width, tile = block.shape
    row = lax.broadcasted_iota(jnp.int32, (rows - width, tile), 0)
    return jnp.concatenate([block, jnp.where(row == 0, 1.0, 0.0).astype(block.dtype)], axis=0)


def split(v):
    high = v.astype(jnp.bfloat16)
    return high, (v - high.astype(jnp.float32)).astype(jnp.bfloat16)


def begin_kernel(features_ref, slot_in_ref, ids_in_ref, start_ref, outgoing_ref, slot_ref, ids_ref, held_ref, arrived):
    blocks, rows, tile = start_ref.shape
    width = features_ref.shape[0]
    copies = [
        pltpu.make_async_copy(ids_in_ref, ids_ref, arrived.at[0]),
        pltpu.make_async_copy(features_ref, held_ref, arrived.at[1]),
        pltpu.make_async_copy(slot_in_ref, slot_ref, arrived.at[2]),
    ]
    for copy in copies:
        copy.start()
    for copy in copies:
        copy.wait()
    for d in range(ids_ref.shape[0]):
        at = pl.multiple_of(ids_ref[d] * tile, tile)
        outgoing_ref[d * width:(d + 1) * width, :] = held_ref[:, pl.ds(at, tile)]
    for b in range(blocks):
        start_ref[b] = framed(held_ref[:, b * tile:(b + 1) * tile], rows)


def step_kernel(index, refs):
    first, last = index == 0, index == ITERS - 1
    refs = list(refs)
    if last:
        held_ref, left = refs.pop(-2), refs.pop()
    current_ref, received_ref, start_ref, slot_ref, ids_ref = refs[:5]
    views_ref = refs.pop()
    if first:
        tiles_ref, next_ref, outgoing_ref, sums_ref, scale_ref, weights_ref = refs[5:]
    elif last:
        scale_ref, weights_ref, past_ref, ranked_ref, sums_ref = refs[5:]
    else:
        scale_ref, weights_ref, past_ref, next_ref, outgoing_ref, sums_ref = refs[5:]
    blocks, rows, tile = current_ref.shape
    width = received_ref.shape[0] // ids_ref.shape[0]
    per_block = weights_ref.shape[0] // (blocks * tile)
    for c in range(blocks + ids_ref.shape[0]):
        v = current_ref[c] if c < blocks else framed(received_ref[(c - blocks) * width:(c - blocks + 1) * width, :], rows)
        views_ref[c, 0:rows], views_ref[c, rows:2 * rows] = split(v)
    square = jnp.zeros((8, tile), jnp.float32)
    copies = []
    for b in range(blocks):
        picked = [views_ref[slot_ref[t]] for t in range(b * per_block, (b + 1) * per_block)]
        lhs = jnp.concatenate(picked, axis=1)
        lhs = jnp.concatenate([lhs, jnp.zeros_like(lhs)], axis=0)
        if first:
            s = None
            for t in range(0, per_block, 2):
                both = []
                for u in range(b * per_block + t, b * per_block + min(t + 2, per_block)):
                    high, low = split(tiles_ref[u].T)
                    weights_ref[u * tile:(u + 1) * tile, 0:tile] = high
                    weights_ref[u * tile:(u + 1) * tile, tile:2 * tile] = low
                    both.append(jnp.concatenate([high, low], axis=1))
                part = jnp.dot(lhs[:, t * tile:(t + 2) * tile], jnp.concatenate(both, axis=0), preferred_element_type=jnp.float32)
                s = part if s is None else s + part
        else:
            s = jnp.dot(lhs, weights_ref[b * per_block * tile:(b + 1) * per_block * tile, :], preferred_element_type=jnp.float32)
        s = s[0:rows] + s[rows:2 * rows]
        s = s[:, 0:tile] + s[:, tile:2 * tile]
        r = slice(b * tile, (b + 1) * tile)
        if first:
            scale = (1.0 - teleport) / (1.0 + s[width:width + 1])
            scale_ref[:, r] = scale
        else:
            scale = scale_ref[:, r]
        old = current_ref[b]
        new = (old + s) * scale + teleport * start_ref[b]
        row = lax.broadcasted_iota(jnp.int32, (rows, tile), 0)
        new = jnp.where(row < width, new, start_ref[b])
        d = new - old
        d = d * d
        for k in range(rows // 8):
            square = square + d[8 * k:8 * k + 8]
        if last:
            held_ref[b] = new[0:width]
            copies.append(pltpu.make_async_copy(held_ref.at[b], ranked_ref.at[:, r], left.at[b]))
            if b:
                copies[b - 1].start()
        else:
            next_ref[b] = new
    row = lax.broadcasted_iota(jnp.int32, (8, tile), 0)
    sums = jnp.where(row == index, jnp.sum(square, axis=0, keepdims=True), 0.0 if first else past_ref[...])
    if last:
        copies[-1].start()
        lane = lax.broadcasted_iota(jnp.int32, (8, tile), 1)
        sums = jnp.where(row == lane, jnp.sum(sums, axis=1, keepdims=True), 0.0)
        sums_ref[...] = jnp.broadcast_to(jnp.sum(sums, axis=0, keepdims=True), sums_ref.shape)
        for copy in copies:
            copy.wait()
    else:
        sums_ref[...] = sums
    if not last:
        for d in range(ids_ref.shape[0]):
            outgoing_ref[d * width:(d + 1) * width, :] = next_ref[ids_ref[d], 0:width]


def shards(features, tiles, tile_slot, send_blocks):
    width, node_count = features.shape
    tile_count, tile, _ = tiles.shape
    blocks = node_count // tile
    peers = lax.axis_size("rows")
    lanes = lax.axis_size("feat")
    halo = peers * send_blocks.shape[2]
    rows = -(-(width + 1) // 8) * 8
    f32 = jnp.float32
    shape = jax.ShapeDtypeStruct

    start, outgoing, slot, ids = pl.pallas_call(
        begin_kernel,
        out_shape=(
            shape((blocks, rows, tile), f32),
            shape((halo * width, tile), f32),
            SMEM(tile_slot.shape, jnp.int32),
            SMEM((halo,), jnp.int32),
        ),
        in_specs=[pl.BlockSpec(memory_space=pltpu.HBM)] * 3,
        out_specs=(WHOLE, WHOLE, SCALARS, SCALARS),
        scratch_shapes=[VMEM(features.shape, f32), pltpu.SemaphoreType.DMA((3,))],
        compiler_params=LIMIT,
        cost_estimate=pl.CostEstimate(flops=20_000_000_000, bytes_accessed=20_000_000, transcendentals=0),
        name="begin",
    )(*(pltpu.with_memory_space_constraint(x, pltpu.HBM) for x in (features, tile_slot, send_blocks.reshape(-1))))

    current = start
    everyone = peers * lanes
    for i in range(ITERS):
        first, last = i == 0, i == ITERS - 1
        received = lax.all_to_all(outgoing.reshape(peers, -1, 1, tile), "rows", split_axis=0, concat_axis=0, tiled=True)
        received = received.reshape(halo * width, tile)
        if last:
            outs = [shape((width, node_count), f32), shape((everyone, tile), f32)]
        else:
            outs = [shape((blocks, rows, tile), f32), shape((halo * width, tile), f32), shape((8, tile), f32)]
        if first:
            outs += [shape((1, node_count), f32), VMEM((tile_count * tile, 2 * tile), jnp.bfloat16)]
        kept = (tiles,) if first else (scale, weights, sums)
        got = pl.pallas_call(
            lambda *refs, i=i: step_kernel(i, refs),
            out_shape=tuple(outs),
            in_specs=[WHOLE] * 3 + [SCALARS] * 2 + [WHOLE] * len(kept),
            out_specs=(pl.BlockSpec(memory_space=pltpu.HBM) if last else WHOLE,) + (WHOLE,) * (len(outs) - 1),
            scratch_shapes=[VMEM((blocks + halo, 2 * rows, tile), jnp.bfloat16)]
            + last * [VMEM((blocks, width, tile), f32), pltpu.SemaphoreType.DMA((blocks,))],
            compiler_params=LIMIT,
            name=f"step{i}",
        )(current, received, start, slot, ids, *kept)
        if first:
            current, outgoing, sums, scale, weights = got
            weights = pltpu.with_memory_space_constraint(weights, VMEM)
        elif last:
            ranked, sums = got
        else:
            current, outgoing, sums = got
    theirs = lax.all_to_all(sums, ("rows", "feat"), split_axis=0, concat_axis=0, tiled=True)
    change = jnp.sum(theirs, axis=0)[:ITERS] / (width * lanes * node_count * peers)
    return ranked, change


def solution(mesh):
    return jax.shard_map(
        shards,
        mesh=mesh,
        in_specs=(P("feat", "rows"), P("rows", None, None), P("rows"), P("rows", None, None)),
        out_specs=(P("feat", "rows"), P()),
        check_vma=False,
    )
```

```python
import functools

import jax
import jax.numpy as jnp
from jax import lax
from jax.experimental import pallas as pl
from jax.experimental.pallas import tpu as pltpu
from jax.sharding import PartitionSpec as P

ITERS = 4


teleport = 0.15

VMEM, SMEM = pltpu.VMEM, pltpu.SMEM
WHOLE = pl.BlockSpec(memory_space=VMEM)
SCALARS = pl.BlockSpec(memory_space=SMEM)
LIMIT = pltpu.CompilerParams(vmem_limit_bytes=20 * 1024 * 1024)


def meeting_order(peers):
    if peers == 8:
        return [5, 6, 4, 3, 7, 2, 1, 0]
    middle = peers // 2 + 1
    return sorted(range(peers), key=lambda i: abs(i - middle))


def framed(block, rows):
    width, tile = block.shape
    row = lax.broadcasted_iota(jnp.int32, (rows - width, tile), 0)
    return jnp.concatenate([block, jnp.where(row == 0, 1.0, 0.0).astype(block.dtype)], axis=0)


def split(v):
    high = v.astype(jnp.bfloat16)
    return high, (v - high.astype(jnp.float32)).astype(jnp.bfloat16)


def begin_kernel(targets, features_ref, slot_in_ref, ids_in_ref, start_ref, outgoing_ref, slot_ref, ids_ref, held_ref, arrived):
    blocks, rows, tile = start_ref.shape
    width = features_ref.shape[0]
    copies = [
        pltpu.make_async_copy(ids_in_ref, ids_ref, arrived.at[0]),
        pltpu.make_async_copy(features_ref, held_ref, arrived.at[1]),
        pltpu.make_async_copy(slot_in_ref, slot_ref, arrived.at[2]),
    ]
    for copy in copies:
        copy.start()
    for copy in copies:
        copy.wait()
    for q, d in enumerate(targets):
        at = pl.multiple_of(ids_ref[d] * tile, tile)
        outgoing_ref[q * width:(q + 1) * width, :] = held_ref[:, pl.ds(at, tile)]
    for b in range(blocks):
        start_ref[b] = framed(held_ref[:, b * tile:(b + 1) * tile], rows)


def step_kernel(index, targets, refs):
    first, last = index == 0, index == ITERS - 1
    refs = list(refs)
    if last:
        held_ref, left = refs.pop(-2), refs.pop()
    current_ref, received_ref, start_ref, slot_ref, ids_ref = refs[:5]
    views_ref = refs.pop()
    if first:
        tiles_ref, next_ref, outgoing_ref, sums_ref, scale_ref, weights_ref = refs[5:]
    elif last:
        scale_ref, weights_ref, past_ref, ranked_ref, sums_ref = refs[5:]
    else:
        scale_ref, weights_ref, past_ref, next_ref, outgoing_ref, sums_ref = refs[5:]
    blocks, rows, tile = current_ref.shape
    width = received_ref.shape[0] // len(targets)
    per_block = weights_ref.shape[0] // (blocks * tile)
    for b in range(blocks):
        views_ref[b, 0:rows], views_ref[b, rows:2 * rows] = split(current_ref[b])
    for q, d in enumerate(targets):
        v = framed(received_ref[q * width:(q + 1) * width, :], rows)
        views_ref[blocks + d, 0:rows], views_ref[blocks + d, rows:2 * rows] = split(v)
    square = jnp.zeros((8, tile), jnp.float32)
    copies = []
    for b in range(blocks):
        picked = [views_ref[slot_ref[t]] for t in range(b * per_block, (b + 1) * per_block)]
        lhs = jnp.concatenate(picked, axis=1)
        lhs = jnp.concatenate([lhs, jnp.zeros_like(lhs)], axis=0)
        if first:
            s = None
            for t in range(0, per_block, 2):
                both = []
                for u in range(b * per_block + t, b * per_block + min(t + 2, per_block)):
                    high, low = split(tiles_ref[u].T)
                    weights_ref[u * tile:(u + 1) * tile, 0:tile] = high
                    weights_ref[u * tile:(u + 1) * tile, tile:2 * tile] = low
                    both.append(jnp.concatenate([high, low], axis=1))
                part = jnp.dot(lhs[:, t * tile:(t + 2) * tile], jnp.concatenate(both, axis=0), preferred_element_type=jnp.float32)
                s = part if s is None else s + part
        else:
            s = jnp.dot(lhs, weights_ref[b * per_block * tile:(b + 1) * per_block * tile, :], preferred_element_type=jnp.float32)
        s = s[0:rows] + s[rows:2 * rows]
        s = s[:, 0:tile] + s[:, tile:2 * tile]
        r = slice(b * tile, (b + 1) * tile)
        if first:
            scale = (1.0 - teleport) / (1.0 + s[width:width + 1])
            scale_ref[:, r] = scale
        else:
            scale = scale_ref[:, r]
        old = current_ref[b]
        new = (old + s) * scale + teleport * start_ref[b]
        row = lax.broadcasted_iota(jnp.int32, (rows, tile), 0)
        new = jnp.where(row < width, new, start_ref[b])
        d = new - old
        d = d * d
        for k in range(rows // 8):
            square = square + d[8 * k:8 * k + 8]
        if last:
            held_ref[b] = new[0:width]
            copies.append(pltpu.make_async_copy(held_ref.at[b], ranked_ref.at[:, r], left.at[b]))
            if b:
                copies[b - 1].start()
        else:
            next_ref[b] = new
    row = lax.broadcasted_iota(jnp.int32, (8, tile), 0)
    sums = jnp.where(row == index, jnp.sum(square, axis=0, keepdims=True), 0.0 if first else past_ref[...])
    if last:
        copies[-1].start()
        lane = lax.broadcasted_iota(jnp.int32, (8, tile), 1)
        sums = jnp.where(row == lane, jnp.sum(sums, axis=1, keepdims=True), 0.0)
        sums_ref[...] = jnp.broadcast_to(jnp.sum(sums, axis=0, keepdims=True), sums_ref.shape)
        for copy in copies:
            copy.wait()
    else:
        sums_ref[...] = sums
    if not last:
        for q, d in enumerate(targets):
            outgoing_ref[q * width:(q + 1) * width, :] = next_ref[ids_ref[d], 0:width]


def shards(features, tiles, tile_slot, send_blocks):
    width, node_count = features.shape
    tile_count, tile, _ = tiles.shape
    blocks = node_count // tile
    peers = lax.axis_size("rows")
    lanes = lax.axis_size("feat")
    slots = send_blocks.shape[2]
    halo = peers * slots
    order = meeting_order(peers)
    targets = [d * slots + k for d in order for k in range(slots)]
    rows = -(-(width + 1) // 8) * 8
    f32 = jnp.float32
    shape = jax.ShapeDtypeStruct

    start, outgoing, slot, ids = pl.pallas_call(
        functools.partial(begin_kernel, targets),
        out_shape=(
            shape((blocks, rows, tile), f32),
            shape((halo * width, tile), f32),
            SMEM(tile_slot.shape, jnp.int32),
            SMEM((halo,), jnp.int32),
        ),
        in_specs=[pl.BlockSpec(memory_space=pltpu.HBM)] * 3,
        out_specs=(WHOLE, WHOLE, SCALARS, SCALARS),
        scratch_shapes=[VMEM(features.shape, f32), pltpu.SemaphoreType.DMA((3,))],
        compiler_params=LIMIT,
        cost_estimate=pl.CostEstimate(flops=20_000_000_000, bytes_accessed=20_000_000, transcendentals=0),
        name="begin",
    )(*(pltpu.with_memory_space_constraint(x, pltpu.HBM) for x in (features, tile_slot, send_blocks.reshape(-1))))

    current = start
    everyone = peers * lanes
    for i in range(ITERS):
        first, last = i == 0, i == ITERS - 1
        received = lax.all_to_all(
            outgoing.reshape(peers, -1, 1, tile), "rows", split_axis=0, concat_axis=0, tiled=True,
            axis_index_groups=[order],
        )
        received = received.reshape(halo * width, tile)
        if last:
            outs = [shape((width, node_count), f32), shape((everyone, tile), f32)]
        else:
            outs = [shape((blocks, rows, tile), f32), shape((halo * width, tile), f32), shape((8, tile), f32)]
        if first:
            outs += [shape((1, node_count), f32), VMEM((tile_count * tile, 2 * tile), jnp.bfloat16)]
        kept = (tiles,) if first else (scale, weights, sums)
        got = pl.pallas_call(
            lambda *refs, i=i: step_kernel(i, targets, refs),
            out_shape=tuple(outs),
            in_specs=[WHOLE] * 3 + [SCALARS] * 2 + [WHOLE] * len(kept),
            out_specs=(pl.BlockSpec(memory_space=pltpu.HBM) if last else WHOLE,) + (WHOLE,) * (len(outs) - 1),
            scratch_shapes=[VMEM((blocks + halo, 2 * rows, tile), jnp.bfloat16)]
            + last * [VMEM((blocks, width, tile), f32), pltpu.SemaphoreType.DMA((blocks,))],
            compiler_params=LIMIT,
            name=f"step{i}",
        )(current, received, start, slot, ids, *kept)
        if first:
            current, outgoing, sums, scale, weights = got
            weights = pltpu.with_memory_space_constraint(weights, VMEM)
        elif last:
            ranked, sums = got
        else:
            current, outgoing, sums = got
    theirs = lax.all_to_all(sums, ("rows", "feat"), split_axis=0, concat_axis=0, tiled=True)
    change = jnp.sum(theirs, axis=0)[:ITERS] / (width * lanes * node_count * peers)
    return ranked, change


def solution(mesh):
    return jax.shard_map(
        shards,
        mesh=mesh,
        in_specs=(P("feat", "rows"), P("rows", None, None), P("rows"), P("rows", None, None)),
        out_specs=(P("feat", "rows"), P()),
        check_vma=False,
    )
```

```python
import functools

import jax
import jax.numpy as jnp
from jax import lax
from jax.experimental import pallas as pl
from jax.experimental.pallas import tpu as pltpu
from jax.sharding import PartitionSpec as P

ITERS = 4


teleport = 0.15

VMEM, SMEM = pltpu.VMEM, pltpu.SMEM
WHOLE = pl.BlockSpec(memory_space=VMEM)
SCALARS = pl.BlockSpec(memory_space=SMEM)
LIMIT = pltpu.CompilerParams(vmem_limit_bytes=20 * 1024 * 1024)


def meeting_order(peers):
    if peers == 8:
        return [5, 6, 4, 3, 7, 2, 1, 0]
    middle = peers // 2 + 1
    return sorted(range(peers), key=lambda i: abs(i - middle))


def framed(block, rows):
    width, tile = block.shape
    row = lax.broadcasted_iota(jnp.int32, (rows - width, tile), 0)
    return jnp.concatenate([block, jnp.where(row == 0, 1.0, 0.0).astype(block.dtype)], axis=0)


def split(v):
    high = v.astype(jnp.bfloat16)
    return high, (v - high.astype(jnp.float32)).astype(jnp.bfloat16)


def turn(tiles, by_product):
    parts = [split(tile) for tile in tiles]
    if by_product:
        flat = jnp.concatenate([jnp.concatenate(half, axis=1) for half in zip(*parts)], axis=0)
        size = flat.shape[1]
        unit = lax.broadcasted_iota(jnp.int32, (size, size), 0) == lax.broadcasted_iota(jnp.int32, (size, size), 1)
        unit = unit.astype(jnp.float32).astype(jnp.bfloat16)
        turned = lax.dot_general(unit, flat, (((1,), (1,)), ((), ())), preferred_element_type=jnp.float32)
        return turned.astype(jnp.bfloat16)
    return jnp.concatenate([jnp.concatenate(split(tile.T), axis=1) for tile in tiles], axis=0)


def begin_kernel(targets, features_ref, slot_in_ref, ids_in_ref, start_ref, outgoing_ref, slot_ref, ids_ref, held_ref, arrived):
    blocks, rows, tile = start_ref.shape
    width = features_ref.shape[0]
    copies = [
        pltpu.make_async_copy(ids_in_ref, ids_ref, arrived.at[0]),
        pltpu.make_async_copy(features_ref, held_ref, arrived.at[1]),
        pltpu.make_async_copy(slot_in_ref, slot_ref, arrived.at[2]),
    ]
    for copy in copies:
        copy.start()
    for copy in copies:
        copy.wait()
    for q, d in enumerate(targets):
        at = pl.multiple_of(ids_ref[d] * tile, tile)
        outgoing_ref[q * width:(q + 1) * width, :] = held_ref[:, pl.ds(at, tile)]
    for b in range(blocks):
        start_ref[b] = framed(held_ref[:, b * tile:(b + 1) * tile], rows)


def step_kernel(index, targets, refs):
    first, last = index == 0, index == ITERS - 1
    refs = list(refs)
    current_ref, received_ref, start_ref, slot_ref, ids_ref = refs[:5]
    views_ref = refs.pop()
    if first:
        tiles_ref, next_ref, outgoing_ref, sums_ref, scale_ref, weights_ref = refs[5:]
    elif last:
        scale_ref, weights_ref, past_ref, ranked_ref, sums_ref = refs[5:]
    else:
        scale_ref, weights_ref, past_ref, next_ref, outgoing_ref, sums_ref = refs[5:]
    blocks, rows, tile = current_ref.shape
    width = received_ref.shape[0] // len(targets)
    per_block = weights_ref.shape[0] // (blocks * tile)
    for b in range(blocks):
        views_ref[b, 0:rows], views_ref[b, rows:2 * rows] = split(current_ref[b])
    for q, d in enumerate(targets):
        v = framed(received_ref[q * width:(q + 1) * width, :], rows)
        views_ref[blocks + d, 0:rows], views_ref[blocks + d, rows:2 * rows] = split(v)
    square = jnp.zeros((8, tile), jnp.float32)
    for b in range(blocks):
        picked = [views_ref[slot_ref[t]] for t in range(b * per_block, (b + 1) * per_block)]
        lhs = jnp.concatenate(picked, axis=1)
        lhs = jnp.concatenate([lhs, jnp.zeros_like(lhs)], axis=0)
        if first:
            s = None
            for t in range(0, per_block, 2):
                at = range(b * per_block + t, b * per_block + min(t + 2, per_block))
                turned = turn([tiles_ref[u] for u in at], by_product=t % 16 == 14)
                weights_ref[at[0] * tile:(at[-1] + 1) * tile, :] = turned
                part = jnp.dot(lhs[:, t * tile:(t + 2) * tile], turned, preferred_element_type=jnp.float32)
                s = part if s is None else s + part
        else:
            s = jnp.dot(lhs, weights_ref[b * per_block * tile:(b + 1) * per_block * tile, :], preferred_element_type=jnp.float32)
        s = s[0:rows] + s[rows:2 * rows]
        s = s[:, 0:tile] + s[:, tile:2 * tile]
        r = slice(b * tile, (b + 1) * tile)
        if first:
            scale = (1.0 - teleport) / (1.0 + s[width:width + 1])
            scale_ref[:, r] = scale
        else:
            scale = scale_ref[:, r]
        old = current_ref[b]
        new = (old + s) * scale + teleport * start_ref[b]
        row = lax.broadcasted_iota(jnp.int32, (rows, tile), 0)
        new = jnp.where(row < width, new, start_ref[b])
        d = new - old
        d = d * d
        for k in range(rows // 8):
            square = square + d[8 * k:8 * k + 8]
        if last:
            ranked_ref[:, r] = new[0:width]
        else:
            next_ref[b] = new
    row = lax.broadcasted_iota(jnp.int32, (8, tile), 0)
    sums = jnp.where(row == index, jnp.sum(square, axis=0, keepdims=True), 0.0 if first else past_ref[...])
    if last:
        lane = lax.broadcasted_iota(jnp.int32, (8, tile), 1)
        sums = jnp.where(row == lane, jnp.sum(sums, axis=1, keepdims=True), 0.0)
        sums_ref[...] = jnp.broadcast_to(jnp.sum(sums, axis=0, keepdims=True), sums_ref.shape)
    else:
        sums_ref[...] = sums
    if not last:
        for q, d in enumerate(targets):
            outgoing_ref[q * width:(q + 1) * width, :] = next_ref[ids_ref[d], 0:width]


def end_kernel(count, theirs_ref, held_ref, ranked_ref, change_ref, mean_ref, left):
    ranked_copy = pltpu.make_async_copy(held_ref, ranked_ref, left.at[0])
    ranked_copy.start()
    sums = jnp.sum(theirs_ref[...], axis=0) / count
    mean_ref[...] = sums[0:mean_ref.shape[0]]
    change_copy = pltpu.make_async_copy(mean_ref, change_ref, left.at[1])
    change_copy.start()
    ranked_copy.wait()
    change_copy.wait()


def shards(features, tiles, tile_slot, send_blocks):
    width, node_count = features.shape
    tile_count, tile, _ = tiles.shape
    blocks = node_count // tile
    peers = lax.axis_size("rows")
    lanes = lax.axis_size("feat")
    slots = send_blocks.shape[2]
    halo = peers * slots
    order = meeting_order(peers)
    targets = [d * slots + k for d in order for k in range(slots)]
    rows = -(-(width + 1) // 8) * 8
    f32 = jnp.float32
    shape = jax.ShapeDtypeStruct

    start, outgoing, slot, ids = pl.pallas_call(
        functools.partial(begin_kernel, targets),
        out_shape=(
            shape((blocks, rows, tile), f32),
            shape((halo * width, tile), f32),
            SMEM(tile_slot.shape, jnp.int32),
            SMEM((halo,), jnp.int32),
        ),
        in_specs=[pl.BlockSpec(memory_space=pltpu.HBM)] * 3,
        out_specs=(WHOLE, WHOLE, SCALARS, SCALARS),
        scratch_shapes=[VMEM(features.shape, f32), pltpu.SemaphoreType.DMA((3,))],
        compiler_params=LIMIT,
        cost_estimate=pl.CostEstimate(flops=20_000_000_000, bytes_accessed=20_000_000, transcendentals=0),
        name="begin",
    )(*(pltpu.with_memory_space_constraint(x, pltpu.HBM) for x in (features, tile_slot, send_blocks.reshape(-1))))

    current = start
    everyone = peers * lanes
    for i in range(ITERS):
        first, last = i == 0, i == ITERS - 1
        received = lax.all_to_all(
            outgoing.reshape(peers, -1, 1, tile), "rows", split_axis=0, concat_axis=0, tiled=True,
            axis_index_groups=[order],
        )
        received = received.reshape(halo * width, tile)
        if last:
            outs = [VMEM((width, node_count), f32), shape((everyone, tile), f32)]
        else:
            outs = [shape((blocks, rows, tile), f32), shape((halo * width, tile), f32), shape((8, tile), f32)]
        if first:
            outs += [shape((1, node_count), f32), VMEM((tile_count * tile, 2 * tile), jnp.bfloat16)]
        kept = (tiles,) if first else (scale, weights, sums)
        got = pl.pallas_call(
            lambda *refs, i=i: step_kernel(i, targets, refs),
            out_shape=tuple(outs),
            in_specs=[WHOLE] * 3 + [SCALARS] * 2 + [WHOLE] * len(kept),
            out_specs=(WHOLE,) * len(outs),
            scratch_shapes=[VMEM((blocks + halo, 2 * rows, tile), jnp.bfloat16)],
            compiler_params=LIMIT,
            name=f"step{i}",
        )(current, received, start, slot, ids, *kept)
        if first:
            current, outgoing, sums, scale, weights = got
            weights = pltpu.with_memory_space_constraint(weights, VMEM)
        elif last:
            ranked, sums = got
        else:
            current, outgoing, sums = got
    theirs = lax.all_to_all(sums, ("rows", "feat"), split_axis=0, concat_axis=0, tiled=True)
    return pl.pallas_call(
        functools.partial(end_kernel, width * lanes * node_count * peers),
        out_shape=(shape((width, node_count), f32), shape((ITERS,), f32)),
        in_specs=[WHOLE, WHOLE],
        out_specs=(pl.BlockSpec(memory_space=pltpu.HBM),) * 2,
        scratch_shapes=[VMEM((ITERS,), f32), pltpu.SemaphoreType.DMA((2,))],
        compiler_params=LIMIT,
        name="end",
    )(theirs, pltpu.with_memory_space_constraint(ranked, VMEM))


def solution(mesh):
    return jax.shard_map(
        shards,
        mesh=mesh,
        in_specs=(P("feat", "rows"), P("rows", None, None), P("rows"), P("rows", None, None)),
        out_specs=(P("feat", "rows"), P()),
        check_vma=False,
    )
```

```python
import functools

import jax
import jax.numpy as jnp
from jax import lax
from jax.experimental import pallas as pl
from jax.experimental.pallas import tpu as pltpu
from jax.sharding import PartitionSpec as P

ITERS = 4


teleport = 0.15

VMEM, SMEM = pltpu.VMEM, pltpu.SMEM
WHOLE = pl.BlockSpec(memory_space=VMEM)
SCALARS = pl.BlockSpec(memory_space=SMEM)
LIMIT = pltpu.CompilerParams(vmem_limit_bytes=20 * 1024 * 1024)


def meeting_order(peers):
    if peers == 8:
        return [5, 7, 3, 2, 6, 4, 1, 0]
    middle = peers // 2 + 1
    return sorted(range(peers), key=lambda i: abs(i - middle))


def framed(block, rows):
    width, tile = block.shape
    row = lax.broadcasted_iota(jnp.int32, (rows - width, tile), 0)
    return jnp.concatenate([block, jnp.where(row == 0, 1.0, 0.0).astype(block.dtype)], axis=0)


def split(v):
    high = v.astype(jnp.bfloat16)
    return high, (v - high.astype(jnp.float32)).astype(jnp.bfloat16)


def stacked(tiles):
    return jnp.concatenate([jnp.concatenate(half, axis=1) for half in zip(*(split(tile) for tile in tiles))], axis=0)


def turned(tiles):
    return jnp.concatenate([jnp.concatenate(split(tile.T), axis=1) for tile in tiles], axis=0)


LATE = (2, 5, 7)


def shelves(blocks, per_block):
    places, filled = {}, {False: 0, True: 0}
    for b in range(blocks):
        for t in range(0, per_block, 2):
            late = t // 2 % 8 in LATE
            places[b, t] = late, filled[late]
            filled[late] += min(2, per_block - t)
    return places, filled[False], filled[True]


def begin_kernel(targets, features_ref, slot_in_ref, ids_in_ref, start_ref, outgoing_ref, slot_ref, ids_ref, held_ref, arrived):
    blocks, rows, tile = start_ref.shape
    width = features_ref.shape[0]
    copies = [
        pltpu.make_async_copy(ids_in_ref, ids_ref, arrived.at[0]),
        pltpu.make_async_copy(slot_in_ref, slot_ref, arrived.at[1]),
    ]
    for b in range(blocks):
        r = slice(b * tile, (b + 1) * tile)
        copies.append(pltpu.make_async_copy(features_ref.at[:, r], held_ref.at[:, r], arrived.at[2 + b]))
    for copy in copies:
        copy.start()
    for copy in copies:
        copy.wait()
    for q, d in enumerate(targets):
        at = pl.multiple_of(ids_ref[d] * tile, tile)
        outgoing_ref[q * width:(q + 1) * width, :] = held_ref[:, pl.ds(at, tile)]
    for b in range(blocks):
        start_ref[b] = framed(held_ref[:, b * tile:(b + 1) * tile], rows)


def step_kernel(index, targets, refs):
    first, last = index == 0, index == ITERS - 1
    refs = list(refs)
    current_ref, received_ref, start_ref, slot_ref, ids_ref = refs[:5]
    views_ref = refs.pop()
    if index == 0:
        tiles_ref, next_ref, outgoing_ref, sums_ref, scale_ref, early_ref = refs[5:]
    elif index == 1:
        scale_ref, early_ref, tiles_ref, past_ref, next_ref, outgoing_ref, sums_ref, late_ref = refs[5:]
    elif last:
        scale_ref, early_ref, late_ref, past_ref, ranked_ref, sums_ref = refs[5:]
    else:
        scale_ref, early_ref, late_ref, past_ref, next_ref, outgoing_ref, sums_ref = refs[5:]
    blocks, rows, tile = current_ref.shape
    width = received_ref.shape[0] // len(targets)
    per_block = slot_ref.shape[0] // blocks
    places, _, _ = shelves(blocks, per_block)
    for b in range(blocks):
        views_ref[b, 0:rows], views_ref[b, rows:2 * rows] = split(current_ref[b])
    for q, d in enumerate(targets):
        v = framed(received_ref[q * width:(q + 1) * width, :], rows)
        views_ref[blocks + d, 0:rows], views_ref[blocks + d, rows:2 * rows] = split(v)
    square = jnp.zeros((8, tile), jnp.float32)
    for b in range(blocks):
        picked = [views_ref[slot_ref[t]] for t in range(b * per_block, (b + 1) * per_block)]
        lhs = jnp.concatenate(picked, axis=1)
        lhs = jnp.concatenate([lhs, jnp.zeros_like(lhs)], axis=0)
        s = None
        for t in range(0, per_block, 2):
            n = min(2, per_block - t)
            late, at = places[b, t]
            view = lhs[:, t * tile:(t + n) * tile]
            if late and index == 0:
                pair = stacked([tiles_ref[b * per_block + t + u] for u in range(n)])
                part = lax.dot_general(view, pair, (((1,), (1,)), ((), ())), preferred_element_type=jnp.float32)
            else:
                shelf_ref = late_ref if late else early_ref
                if late == (index == 1) and index < 2:
                    pair = turned([tiles_ref[b * per_block + t + u] for u in range(n)])
                    shelf_ref[at * tile:(at + n) * tile, :] = pair
                else:
                    pair = shelf_ref[at * tile:(at + n) * tile, :]
                part = jnp.dot(view, pair, preferred_element_type=jnp.float32)
            s = part if s is None else s + part
        s = s[0:rows] + s[rows:2 * rows]
        s = s[:, 0:tile] + s[:, tile:2 * tile]
        r = slice(b * tile, (b + 1) * tile)
        if first:
            scale = (1.0 - teleport) / (1.0 + s[width:width + 1])
            scale_ref[:, r] = scale
        else:
            scale = scale_ref[:, r]
        old = current_ref[b]
        new = (old + s) * scale + teleport * start_ref[b]
        row = lax.broadcasted_iota(jnp.int32, (rows, tile), 0)
        new = jnp.where(row < width, new, start_ref[b])
        d = new - old
        d = d * d
        for k in range(rows // 8):
            square = square + d[8 * k:8 * k + 8]
        if last:
            ranked_ref[:, r] = new[0:width]
        else:
            next_ref[b] = new
    row = lax.broadcasted_iota(jnp.int32, (8, tile), 0)
    sums = jnp.where(row == index, jnp.sum(square, axis=0, keepdims=True), 0.0 if first else past_ref[...])
    if last:
        lane = lax.broadcasted_iota(jnp.int32, (8, tile), 1)
        sums = jnp.where(row == lane, jnp.sum(sums, axis=1, keepdims=True), 0.0)
        sums_ref[...] = jnp.broadcast_to(jnp.sum(sums, axis=0, keepdims=True), sums_ref.shape)
    else:
        sums_ref[...] = sums
    if not last:
        for q, d in enumerate(targets):
            outgoing_ref[q * width:(q + 1) * width, :] = next_ref[ids_ref[d], 0:width]


def end_kernel(count, theirs_ref, held_ref, ranked_ref, change_ref, mean_ref, left):
    ranked_copy = pltpu.make_async_copy(held_ref, ranked_ref, left.at[0])
    ranked_copy.start()
    sums = jnp.sum(theirs_ref[...], axis=0) / count
    mean_ref[...] = sums[0:mean_ref.shape[0]]
    change_copy = pltpu.make_async_copy(mean_ref, change_ref, left.at[1])
    change_copy.start()
    ranked_copy.wait()
    change_copy.wait()


def shards(features, tiles, tile_slot, send_blocks):
    width, node_count = features.shape
    tile_count, tile, _ = tiles.shape
    blocks = node_count // tile
    peers = lax.axis_size("rows")
    lanes = lax.axis_size("feat")
    slots = send_blocks.shape[2]
    halo = peers * slots
    order = meeting_order(peers)
    targets = [d * slots + k for d in order for k in range(slots)]
    rows = -(-(width + 1) // 8) * 8
    f32 = jnp.float32
    shape = jax.ShapeDtypeStruct

    start, outgoing, slot, ids = pl.pallas_call(
        functools.partial(begin_kernel, targets),
        out_shape=(
            shape((blocks, rows, tile), f32),
            shape((halo * width, tile), f32),
            SMEM(tile_slot.shape, jnp.int32),
            SMEM((halo,), jnp.int32),
        ),
        in_specs=[pl.BlockSpec(memory_space=pltpu.HBM)] * 3,
        out_specs=(WHOLE, WHOLE, SCALARS, SCALARS),
        scratch_shapes=[VMEM(features.shape, f32), pltpu.SemaphoreType.DMA((2 + blocks,))],
        compiler_params=LIMIT,
        cost_estimate=pl.CostEstimate(flops=20_000_000_000, bytes_accessed=20_000_000, transcendentals=0),
        name="begin",
    )(*(pltpu.with_memory_space_constraint(x, pltpu.HBM) for x in (features, tile_slot, send_blocks.reshape(-1))))

    current = start
    everyone = peers * lanes
    _, early_count, late_count = shelves(blocks, tile_count // blocks)
    for i in range(ITERS):
        first, last = i == 0, i == ITERS - 1
        received = lax.all_to_all(
            outgoing.reshape(peers, -1, 1, tile), "rows", split_axis=0, concat_axis=0, tiled=True,
            axis_index_groups=[order],
        )
        received = received.reshape(halo * width, tile)
        if last:
            outs = [VMEM((width, node_count), f32), shape((everyone, tile), f32)]
        else:
            outs = [shape((blocks, rows, tile), f32), shape((halo * width, tile), f32), shape((8, tile), f32)]
        if first:
            outs += [shape((1, node_count), f32), VMEM((early_count * tile, 2 * tile), jnp.bfloat16)]
        if i == 1:
            outs += [VMEM((late_count * tile, 2 * tile), jnp.bfloat16)]
        kept = (tiles,) if first else (scale, early, tiles, sums) if i == 1 else (scale, early, late, sums)
        got = pl.pallas_call(
            lambda *refs, i=i: step_kernel(i, targets, refs),
            out_shape=tuple(outs),
            in_specs=[WHOLE] * 3 + [SCALARS] * 2 + [WHOLE] * len(kept),
            out_specs=(WHOLE,) * len(outs),
            scratch_shapes=[VMEM((blocks + halo, 2 * rows, tile), jnp.bfloat16)],
            compiler_params=LIMIT,
            name=f"step{i}",
        )(current, received, start, slot, ids, *kept)
        if first:
            current, outgoing, sums, scale, early = got
            early = pltpu.with_memory_space_constraint(early, VMEM)
        elif i == 1:
            current, outgoing, sums, late = got
            late = pltpu.with_memory_space_constraint(late, VMEM)
        elif last:
            ranked, sums = got
        else:
            current, outgoing, sums = got
    theirs = lax.all_to_all(sums, ("rows", "feat"), split_axis=0, concat_axis=0, tiled=True)
    return pl.pallas_call(
        functools.partial(end_kernel, width * lanes * node_count * peers),
        out_shape=(shape((width, node_count), f32), shape((ITERS,), f32)),
        in_specs=[WHOLE, WHOLE],
        out_specs=(pl.BlockSpec(memory_space=pltpu.HBM),) * 2,
        scratch_shapes=[VMEM((ITERS,), f32), pltpu.SemaphoreType.DMA((2,))],
        compiler_params=LIMIT,
        name="end",
    )(theirs, pltpu.with_memory_space_constraint(ranked, VMEM))


def solution(mesh):
    return jax.shard_map(
        shards,
        mesh=mesh,
        in_specs=(P("feat", "rows"), P("rows", None, None), P("rows"), P("rows", None, None)),
        out_specs=(P("feat", "rows"), P()),
        check_vma=False,
    )
```

```python
import functools

import jax
import jax.numpy as jnp
from jax import lax
from jax.experimental import pallas as pl
from jax.experimental.pallas import tpu as pltpu
from jax.sharding import PartitionSpec as P

ITERS = 4


teleport = 0.15

VMEM, SMEM = pltpu.VMEM, pltpu.SMEM
WHOLE = pl.BlockSpec(memory_space=VMEM)
SCALARS = pl.BlockSpec(memory_space=SMEM)
LIMIT = pltpu.CompilerParams(vmem_limit_bytes=20 * 1024 * 1024)


def meeting_order(peers):
    if peers == 8:
        return [5, 7, 3, 2, 6, 4, 1, 0]
    middle = peers // 2 + 1
    return sorted(range(peers), key=lambda i: abs(i - middle))


def framed(block, rows):
    width, tile = block.shape
    row = lax.broadcasted_iota(jnp.int32, (rows - width, tile), 0)
    return jnp.concatenate([block, jnp.where(row == 0, 1.0, 0.0).astype(block.dtype)], axis=0)


def split(v):
    high = v.astype(jnp.bfloat16)
    return high, (v - high.astype(jnp.float32)).astype(jnp.bfloat16)


def stacked(tiles):
    return jnp.concatenate([jnp.concatenate(half, axis=1) for half in zip(*(split(tile) for tile in tiles))], axis=0)


def turned(tiles):
    return jnp.concatenate([jnp.concatenate(split(tile.T), axis=1) for tile in tiles], axis=0)


LATE = (2, 5, 7)


def shelves(blocks, per_block):
    places, filled = {}, {False: 0, True: 0}
    for b in range(blocks):
        for t in range(0, per_block, 2):
            late = t // 2 % 8 in LATE
            places[b, t] = late, filled[late]
            filled[late] += min(2, per_block - t)
    return places, filled[False], filled[True]


def begin_kernel(targets, features_ref, slot_in_ref, ids_in_ref, start_ref, outgoing_ref, slot_ref, ids_ref, held_ref, arrived):
    blocks, rows, tile = start_ref.shape
    width = features_ref.shape[0]
    copies = [
        pltpu.make_async_copy(ids_in_ref, ids_ref, arrived.at[0]),
        pltpu.make_async_copy(slot_in_ref, slot_ref, arrived.at[1]),
    ]
    for b in range(blocks):
        r = slice(b * tile, (b + 1) * tile)
        copies.append(pltpu.make_async_copy(features_ref.at[:, r], held_ref.at[:, r], arrived.at[2 + b]))
    for copy in copies:
        copy.start(priority=1)
    for copy in copies:
        copy.wait()
    for q, d in enumerate(targets):
        at = pl.multiple_of(ids_ref[d] * tile, tile)
        outgoing_ref[q * width:(q + 1) * width, :] = held_ref[:, pl.ds(at, tile)]
    for b in range(blocks):
        start_ref[b] = framed(held_ref[:, b * tile:(b + 1) * tile], rows)


def step_kernel(index, targets, refs):
    first, last = index == 0, index == ITERS - 1
    refs = list(refs)
    current_ref, received_ref, start_ref, slot_ref, ids_ref = refs[:5]
    views_ref = refs.pop()
    if index == 0:
        tiles_ref, next_ref, outgoing_ref, sums_ref, scale_ref, early_ref = refs[5:]
    elif index == 1:
        scale_ref, early_ref, tiles_ref, past_ref, next_ref, outgoing_ref, sums_ref, late_ref = refs[5:]
    elif last:
        scale_ref, early_ref, late_ref, past_ref, ranked_ref, sums_ref = refs[5:]
    else:
        scale_ref, early_ref, late_ref, past_ref, next_ref, outgoing_ref, sums_ref = refs[5:]
    blocks, rows, tile = current_ref.shape
    width = received_ref.shape[0] // len(targets)
    per_block = slot_ref.shape[0] // blocks
    places, _, _ = shelves(blocks, per_block)
    for b in range(blocks):
        views_ref[b, 0:rows], views_ref[b, rows:2 * rows] = split(current_ref[b])
    for q, d in enumerate(targets):
        v = framed(received_ref[q * width:(q + 1) * width, :], rows)
        views_ref[blocks + d, 0:rows], views_ref[blocks + d, rows:2 * rows] = split(v)
    square = jnp.zeros((8, tile), jnp.float32)
    for b in range(blocks):
        picked = [views_ref[slot_ref[t]] for t in range(b * per_block, (b + 1) * per_block)]
        lhs = jnp.concatenate(picked, axis=1)
        lhs = jnp.concatenate([lhs, jnp.zeros_like(lhs)], axis=0)
        s = None
        for t in range(0, per_block, 2):
            n = min(2, per_block - t)
            late, at = places[b, t]
            view = lhs[:, t * tile:(t + n) * tile]
            if late and index == 0:
                pair = stacked([tiles_ref[b * per_block + t + u] for u in range(n)])
                part = lax.dot_general(view, pair, (((1,), (1,)), ((), ())), preferred_element_type=jnp.float32)
            else:
                shelf_ref = late_ref if late else early_ref
                if late == (index == 1) and index < 2:
                    pair = turned([tiles_ref[b * per_block + t + u] for u in range(n)])
                    shelf_ref[at * tile:(at + n) * tile, :] = pair
                else:
                    pair = shelf_ref[at * tile:(at + n) * tile, :]
                part = jnp.dot(view, pair, preferred_element_type=jnp.float32)
            s = part if s is None else s + part
        s = s[0:rows] + s[rows:2 * rows]
        s = s[:, 0:tile] + s[:, tile:2 * tile]
        r = slice(b * tile, (b + 1) * tile)
        if first:
            scale = (1.0 - teleport) / (1.0 + s[width:width + 1])
            scale_ref[:, r] = scale
        else:
            scale = scale_ref[:, r]
        old = current_ref[b]
        new = (old + s) * scale + teleport * start_ref[b]
        row = lax.broadcasted_iota(jnp.int32, (rows, tile), 0)
        new = jnp.where(row < width, new, start_ref[b])
        d = new - old
        d = d * d
        for k in range(rows // 8):
            square = square + d[8 * k:8 * k + 8]
        if last:
            ranked_ref[:, r] = new[0:width]
        else:
            next_ref[b] = new
    row = lax.broadcasted_iota(jnp.int32, (8, tile), 0)
    sums = jnp.where(row == index, jnp.sum(square, axis=0, keepdims=True), 0.0 if first else past_ref[...])
    if last:
        lane = lax.broadcasted_iota(jnp.int32, (8, tile), 1)
        sums = jnp.where(row == lane, jnp.sum(sums, axis=1, keepdims=True), 0.0)
        sums_ref[...] = jnp.broadcast_to(jnp.sum(sums, axis=0, keepdims=True), sums_ref.shape)
    else:
        sums_ref[...] = sums
    if not last:
        for q, d in enumerate(targets):
            outgoing_ref[q * width:(q + 1) * width, :] = next_ref[ids_ref[d], 0:width]


def end_kernel(count, theirs_ref, held_ref, ranked_ref, change_ref, mean_ref, left):
    ranked_copy = pltpu.make_async_copy(held_ref, ranked_ref, left.at[0])
    ranked_copy.start()
    sums = jnp.sum(theirs_ref[...], axis=0) / count
    mean_ref[...] = sums[0:mean_ref.shape[0]]
    change_copy = pltpu.make_async_copy(mean_ref, change_ref, left.at[1])
    change_copy.start()
    ranked_copy.wait()
    change_copy.wait()


def shards(features, tiles, tile_slot, send_blocks):
    width, node_count = features.shape
    tile_count, tile, _ = tiles.shape
    blocks = node_count // tile
    peers = lax.axis_size("rows")
    lanes = lax.axis_size("feat")
    slots = send_blocks.shape[2]
    halo = peers * slots
    order = meeting_order(peers)
    targets = [d * slots + k for d in order for k in range(slots)]
    rows = -(-(width + 1) // 8) * 8
    f32 = jnp.float32
    shape = jax.ShapeDtypeStruct

    start, outgoing, slot, ids = pl.pallas_call(
        functools.partial(begin_kernel, targets),
        out_shape=(
            shape((blocks, rows, tile), f32),
            shape((halo * width, tile), f32),
            SMEM(tile_slot.shape, jnp.int32),
            SMEM((halo,), jnp.int32),
        ),
        in_specs=[pl.BlockSpec(memory_space=pltpu.HBM)] * 3,
        out_specs=(WHOLE, WHOLE, SCALARS, SCALARS),
        scratch_shapes=[VMEM(features.shape, f32), pltpu.SemaphoreType.DMA((2 + blocks,))],
        compiler_params=LIMIT,
        cost_estimate=pl.CostEstimate(flops=20_000_000_000, bytes_accessed=20_000_000, transcendentals=0),
        name="begin",
    )(*(pltpu.with_memory_space_constraint(x, pltpu.HBM) for x in (features, tile_slot, send_blocks.reshape(-1))))

    current = start
    everyone = peers * lanes
    _, early_count, late_count = shelves(blocks, tile_count // blocks)
    for i in range(ITERS):
        first, last = i == 0, i == ITERS - 1
        received = lax.all_to_all(
            outgoing.reshape(peers, -1, 1, tile), "rows", split_axis=0, concat_axis=0, tiled=True,
            axis_index_groups=[order],
        )
        received = received.reshape(halo * width, tile)
        if last:
            outs = [VMEM((width, node_count), f32), shape((everyone, tile), f32)]
        else:
            outs = [shape((blocks, rows, tile), f32), shape((halo * width, tile), f32), shape((8, tile), f32)]
        if first:
            outs += [shape((1, node_count), f32), VMEM((early_count * tile, 2 * tile), jnp.bfloat16)]
        if i == 1:
            outs += [VMEM((late_count * tile, 2 * tile), jnp.bfloat16)]
        kept = (tiles,) if first else (scale, early, tiles, sums) if i == 1 else (scale, early, late, sums)
        got = pl.pallas_call(
            lambda *refs, i=i: step_kernel(i, targets, refs),
            out_shape=tuple(outs),
            in_specs=[WHOLE] * 3 + [SCALARS] * 2 + [WHOLE] * len(kept),
            out_specs=(WHOLE,) * len(outs),
            scratch_shapes=[VMEM((blocks + halo, 2 * rows, tile), jnp.bfloat16)],
            compiler_params=LIMIT,
            name=f"step{i}",
        )(current, received, start, slot, ids, *kept)
        if first:
            current, outgoing, sums, scale, early = got
            early = pltpu.with_memory_space_constraint(early, VMEM)
        elif i == 1:
            current, outgoing, sums, late = got
            late = pltpu.with_memory_space_constraint(late, VMEM)
        elif last:
            ranked, sums = got
        else:
            current, outgoing, sums = got
    theirs = lax.all_to_all(sums, ("rows", "feat"), split_axis=0, concat_axis=0, tiled=True)
    return pl.pallas_call(
        functools.partial(end_kernel, width * lanes * node_count * peers),
        out_shape=(shape((width, node_count), f32), shape((ITERS,), f32)),
        in_specs=[WHOLE, WHOLE],
        out_specs=(pl.BlockSpec(memory_space=pltpu.HBM),) * 2,
        scratch_shapes=[VMEM((ITERS,), f32), pltpu.SemaphoreType.DMA((2,))],
        compiler_params=LIMIT,
        name="end",
    )(theirs, pltpu.with_memory_space_constraint(ranked, VMEM))


def solution(mesh):
    return jax.shard_map(
        shards,
        mesh=mesh,
        in_specs=(P("feat", "rows"), P("rows", None, None), P("rows"), P("rows", None, None)),
        out_specs=(P("feat", "rows"), P()),
        check_vma=False,
    )
```

```python
import functools

import jax
import jax.numpy as jnp
from jax import lax
from jax.experimental import pallas as pl
from jax.experimental.pallas import tpu as pltpu
from jax.sharding import PartitionSpec as P

ITERS = 4


teleport = 0.15

VMEM, SMEM = pltpu.VMEM, pltpu.SMEM
WHOLE = pl.BlockSpec(memory_space=VMEM)
SCALARS = pl.BlockSpec(memory_space=SMEM)
LIMIT = pltpu.CompilerParams(vmem_limit_bytes=20 * 1024 * 1024)


def meeting_order(peers):
    if peers == 8:
        return [5, 7, 3, 2, 6, 4, 1, 0]
    middle = peers // 2 + 1
    return sorted(range(peers), key=lambda i: abs(i - middle))


def framed(block, rows):
    width, tile = block.shape
    row = lax.broadcasted_iota(jnp.int32, (rows - width, tile), 0)
    return jnp.concatenate([block, jnp.where(row == 0, 1.0, 0.0).astype(block.dtype)], axis=0)


def split(v):
    high = v.astype(jnp.bfloat16)
    return high, (v - high.astype(jnp.float32)).astype(jnp.bfloat16)


def stacked(tiles):
    return jnp.concatenate([jnp.concatenate(half, axis=1) for half in zip(*(split(tile) for tile in tiles))], axis=0)


def turned(tiles):
    return jnp.concatenate([jnp.concatenate(split(tile.T), axis=1) for tile in tiles], axis=0)


LATE = (2, 5, 7)


def shelves(blocks, per_block):
    places, filled = {}, {False: 0, True: 0}
    for b in range(blocks):
        for t in range(0, per_block, 2):
            late = t // 2 % 8 in LATE
            places[b, t] = late, filled[late]
            filled[late] += min(2, per_block - t)
    return places, filled[False], filled[True]


def begin_kernel(targets, features_ref, slot_in_ref, ids_in_ref, start_ref, outgoing_ref, slot_ref, ids_ref, held_ref, arrived):
    blocks, rows, tile = start_ref.shape
    width = features_ref.shape[0]
    copies = [
        pltpu.make_async_copy(ids_in_ref, ids_ref, arrived.at[0]),
        pltpu.make_async_copy(slot_in_ref, slot_ref, arrived.at[1]),
    ]
    for b in range(blocks):
        r = slice(b * tile, (b + 1) * tile)
        copies.append(pltpu.make_async_copy(features_ref.at[:, r], held_ref.at[:, r], arrived.at[2 + b]))
    for copy in copies:
        copy.start(priority=1)
    for copy in copies[:1] + copies[2:]:
        copy.wait()
    for q, d in enumerate(targets):
        at = pl.multiple_of(ids_ref[d] * tile, tile)
        outgoing_ref[q * width:(q + 1) * width, :] = held_ref[:, pl.ds(at, tile)]
    for b in range(blocks):
        start_ref[b] = framed(held_ref[:, b * tile:(b + 1) * tile], rows)
    copies[1].wait()


def step_kernel(index, targets, refs):
    first, last = index == 0, index == ITERS - 1
    refs = list(refs)
    current_ref, received_ref, start_ref, slot_ref, ids_ref = refs[:5]
    views_ref = refs.pop()
    if index == 0:
        tiles_ref, next_ref, outgoing_ref, sums_ref, scale_ref, early_ref = refs[5:]
    elif index == 1:
        scale_ref, early_ref, tiles_ref, past_ref, next_ref, outgoing_ref, sums_ref, late_ref = refs[5:]
    elif last:
        scale_ref, early_ref, late_ref, past_ref, ranked_ref, sums_ref = refs[5:]
    else:
        scale_ref, early_ref, late_ref, past_ref, next_ref, outgoing_ref, sums_ref = refs[5:]
    blocks, rows, tile = current_ref.shape
    width = received_ref.shape[0] // len(targets)
    per_block = slot_ref.shape[0] // blocks
    places, _, _ = shelves(blocks, per_block)
    for b in range(blocks):
        views_ref[b, 0:rows], views_ref[b, rows:2 * rows] = split(current_ref[b])
    for q, d in enumerate(targets):
        v = framed(received_ref[q * width:(q + 1) * width, :], rows)
        views_ref[blocks + d, 0:rows], views_ref[blocks + d, rows:2 * rows] = split(v)
    square = jnp.zeros((8, tile), jnp.float32)
    for b in range(blocks):
        picked = [views_ref[slot_ref[t]] for t in range(b * per_block, (b + 1) * per_block)]
        lhs = jnp.concatenate(picked, axis=1)
        lhs = jnp.concatenate([lhs, jnp.zeros_like(lhs)], axis=0)
        s = None
        for t in range(0, per_block, 2):
            n = min(2, per_block - t)
            late, at = places[b, t]
            view = lhs[:, t * tile:(t + n) * tile]
            if late and index == 0:
                pair = stacked([tiles_ref[b * per_block + t + u] for u in range(n)])
                part = lax.dot_general(view, pair, (((1,), (1,)), ((), ())), preferred_element_type=jnp.float32)
            else:
                shelf_ref = late_ref if late else early_ref
                if late == (index == 1) and index < 2:
                    pair = turned([tiles_ref[b * per_block + t + u] for u in range(n)])
                    shelf_ref[at * tile:(at + n) * tile, :] = pair
                else:
                    pair = shelf_ref[at * tile:(at + n) * tile, :]
                part = jnp.dot(view, pair, preferred_element_type=jnp.float32)
            s = part if s is None else s + part
        s = s[0:rows] + s[rows:2 * rows]
        s = s[:, 0:tile] + s[:, tile:2 * tile]
        r = slice(b * tile, (b + 1) * tile)
        if first:
            scale = (1.0 - teleport) / (1.0 + s[width:width + 1])
            scale_ref[:, r] = scale
        else:
            scale = scale_ref[:, r]
        old = current_ref[b]
        new = (old + s) * scale + teleport * start_ref[b]
        row = lax.broadcasted_iota(jnp.int32, (rows, tile), 0)
        new = jnp.where(row < width, new, start_ref[b])
        d = new - old
        d = d * d
        for k in range(rows // 8):
            square = square + d[8 * k:8 * k + 8]
        if last:
            ranked_ref[:, r] = new[0:width]
        else:
            next_ref[b] = new
    row = lax.broadcasted_iota(jnp.int32, (8, tile), 0)
    sums = jnp.where(row == index, jnp.sum(square, axis=0, keepdims=True), 0.0 if first else past_ref[...])
    if last:
        lane = lax.broadcasted_iota(jnp.int32, (8, tile), 1)
        sums = jnp.where(row == lane, jnp.sum(sums, axis=1, keepdims=True), 0.0)
        sums_ref[...] = jnp.broadcast_to(jnp.sum(sums, axis=0, keepdims=True), sums_ref.shape)
    else:
        sums_ref[...] = sums
    if not last:
        for q, d in enumerate(targets):
            outgoing_ref[q * width:(q + 1) * width, :] = next_ref[ids_ref[d], 0:width]


def end_kernel(count, theirs_ref, held_ref, ranked_ref, change_ref, mean_ref, left):
    ranked_copy = pltpu.make_async_copy(held_ref, ranked_ref, left.at[0])
    ranked_copy.start()
    sums = jnp.sum(theirs_ref[...], axis=0) / count
    mean_ref[...] = sums[0:mean_ref.shape[0]]
    change_copy = pltpu.make_async_copy(mean_ref, change_ref, left.at[1])
    change_copy.start()
    ranked_copy.wait()
    change_copy.wait()


def shards(features, tiles, tile_slot, send_blocks):
    width, node_count = features.shape
    tile_count, tile, _ = tiles.shape
    blocks = node_count // tile
    peers = lax.axis_size("rows")
    lanes = lax.axis_size("feat")
    slots = send_blocks.shape[2]
    halo = peers * slots
    order = meeting_order(peers)
    targets = [d * slots + k for d in order for k in range(slots)]
    rows = -(-(width + 1) // 8) * 8
    f32 = jnp.float32
    shape = jax.ShapeDtypeStruct

    start, outgoing, slot, ids = pl.pallas_call(
        functools.partial(begin_kernel, targets),
        out_shape=(
            shape((blocks, rows, tile), f32),
            shape((halo * width, tile), f32),
            SMEM(tile_slot.shape, jnp.int32),
            SMEM((halo,), jnp.int32),
        ),
        in_specs=[pl.BlockSpec(memory_space=pltpu.HBM)] * 3,
        out_specs=(WHOLE, WHOLE, SCALARS, SCALARS),
        scratch_shapes=[VMEM(features.shape, f32), pltpu.SemaphoreType.DMA((2 + blocks,))],
        compiler_params=LIMIT,
        cost_estimate=pl.CostEstimate(flops=20_000_000_000, bytes_accessed=20_000_000, transcendentals=0),
        name="begin",
    )(*(pltpu.with_memory_space_constraint(x, pltpu.HBM) for x in (features, tile_slot, send_blocks.reshape(-1))))

    current = start
    everyone = peers * lanes
    _, early_count, late_count = shelves(blocks, tile_count // blocks)
    for i in range(ITERS):
        first, last = i == 0, i == ITERS - 1
        received = lax.all_to_all(
            outgoing.reshape(peers, -1, 1, tile), "rows", split_axis=0, concat_axis=0, tiled=True,
            axis_index_groups=[order],
        )
        received = received.reshape(halo * width, tile)
        if last:
            outs = [VMEM((width, node_count), f32), shape((everyone, tile), f32)]
        else:
            outs = [shape((blocks, rows, tile), f32), shape((halo * width, tile), f32), shape((8, tile), f32)]
        if first:
            outs += [shape((1, node_count), f32), VMEM((early_count * tile, 2 * tile), jnp.bfloat16)]
        if i == 1:
            outs += [VMEM((late_count * tile, 2 * tile), jnp.bfloat16)]
        kept = (tiles,) if first else (scale, early, tiles, sums) if i == 1 else (scale, early, late, sums)
        got = pl.pallas_call(
            lambda *refs, i=i: step_kernel(i, targets, refs),
            out_shape=tuple(outs),
            in_specs=[WHOLE] * 3 + [SCALARS] * 2 + [WHOLE] * len(kept),
            out_specs=(WHOLE,) * len(outs),
            scratch_shapes=[VMEM((blocks + halo, 2 * rows, tile), jnp.bfloat16)],
            compiler_params=LIMIT,
            name=f"step{i}",
        )(current, received, start, slot, ids, *kept)
        if first:
            current, outgoing, sums, scale, early = got
            early = pltpu.with_memory_space_constraint(early, VMEM)
        elif i == 1:
            current, outgoing, sums, late = got
            late = pltpu.with_memory_space_constraint(late, VMEM)
        elif last:
            ranked, sums = got
        else:
            current, outgoing, sums = got
    theirs = lax.all_to_all(sums, ("rows", "feat"), split_axis=0, concat_axis=0, tiled=True)
    return pl.pallas_call(
        functools.partial(end_kernel, width * lanes * node_count * peers),
        out_shape=(shape((width, node_count), f32), shape((ITERS,), f32)),
        in_specs=[WHOLE, WHOLE],
        out_specs=(pl.BlockSpec(memory_space=pltpu.HBM),) * 2,
        scratch_shapes=[VMEM((ITERS,), f32), pltpu.SemaphoreType.DMA((2,))],
        compiler_params=LIMIT,
        name="end",
    )(theirs, pltpu.with_memory_space_constraint(ranked, VMEM))


def solution(mesh):
    return jax.shard_map(
        shards,
        mesh=mesh,
        in_specs=(P("feat", "rows"), P("rows", None, None), P("rows"), P("rows", None, None)),
        out_specs=(P("feat", "rows"), P()),
        check_vma=False,
    )
```
